32 devices in a mesh: row: 8 (over z, x), col: 4 (over y, core).
Axes of the slice: x: 2, y: 2, z: 4, core: 2. Of those that a mesh axis runs over, the one named last changes fastest.
Arguments:
- momentum: float32 [5120, 13312], P('row', 'col')
- gradient: float32 [5120, 13312], P('row', 'col'), may hold values from -6 to 6
Outputs:
- new_momentum: float32 [5120, 13312], P('row', 'col')
- update: float32 [5120, 13312], P('row', 'col')
The draws below stay inside these ranges and needn't reach their ends.
All inputs are finite; a program needn't handle non-finite values.
Results may differ from the reference program's by a relative error of at most 0.00073.
The reference program's roundings to bfloat16 on the way (of `rounded` and `gram_rounded`) count: a program that leaves them out, or rounds other values in their place, can miss the bound.
Values may be sent and summed in bfloat16 or wider, within the bound.
No kernel may reach another device: no remote copies, remote signals or barrier semaphores. Data moves between devices by JAX's collectives and lax.ppermute only.
A program may use at most 128 MiB of HBM per device.

```python
import jax
import jax.numpy as jnp

D = 5120
FF_WIN = 13312


def draw_momentum(key, part):
    noise_key = jax.random.fold_in(key, 11)
    return jax.random.normal(noise_key, (D, FF_WIN), jnp.float32)


def steps_of(rng, extent, pieces, least, largest):
    gain, own = 1.0, jax.random.fold_in(rng, 6)
    for axis_at, parts in pieces:
        heights = jnp.exp(jax.random.uniform(jax.random.fold_in(own, axis_at), (parts,), jnp.float32, least / len(pieces), largest / len(pieces)))
        gain = gain * jnp.repeat(heights, extent[axis_at] // parts).reshape([-1 if axis == axis_at else 1 for axis in range(len(extent))])
    return gain


def bell_draw(own_key, extent, width, bound, cuts=(), held_as=jnp.bfloat16):
    factor_of = steps_of(own_key, extent, cuts, -0.22, 0.18) if cuts else 1.0
    array = jax.random.normal(own_key, extent, jnp.float32) * width * factor_of
    return jnp.minimum(jnp.maximum(array, -bound), bound).astype(held_as)


def setup_inputs(seed: int = 0) -> dict:
    key_of = jax.random.split(jax.random.key(seed), 3)
    return {
        "momentum": draw_momentum(jax.random.fold_in(key_of[2], 71), 0),
        "gradient": bell_draw(key_of[1], (D, FF_WIN), 0.5, 6.0, ((0, 8), (1, 4)), jnp.float32),
    }


def reference(momentum, gradient):
    new_momentum = 0.95 * momentum + gradient
    squares = jnp.sum(new_momentum * new_momentum)
    normed = new_momentum / (jnp.sqrt(3.0 * squares / D) + 1e-07)
    rounded = normed.astype(jnp.bfloat16)
    gram = jnp.dot(rounded, rounded.T, preferred_element_type=jnp.float32)
    gram_rounded = gram.astype(jnp.bfloat16)
    product = jnp.dot(gram_rounded, rounded, preferred_element_type=jnp.float32)
    update = (1.5 * normed - 0.5 * product) * jnp.sqrt(jnp.float32(3 * FF_WIN))
    return (new_momentum, update)
```

```python
import jax
import jax.numpy as jnp
from jax import lax
from jax.experimental import pallas as pl
from jax.experimental.pallas import tpu as pltpu
from jax.sharding import PartitionSpec as P


D = 5120
FF_WIN = 13312


def cycle(mesh):
    places = [tuple(d.coords) for d in mesh.devices[:, 0]]
    n = len(places)
    first = [a != b for a, b in zip(places[0], places[1 % n])]
    minor = n
    for i, place in enumerate(places):
        if any(a != b and not f for a, b, f in zip(place, places[0], first)):
            minor = i
            break
    major = n // minor
    order = []
    for i in range(major):
        along = range(1, minor) if i % 2 == 0 else range(minor - 1, 0, -1)
        order += [i * minor + j for j in along]
    order += [i * minor for i in range(major - 1, -1, -1)]
    return order


def flip(x, bit, n, axis):
    return lax.ppermute(x, axis, [(i, i ^ bit) for i in range(n)])


def bits_of(n):
    return [1 << k for k in range(n.bit_length() - 1)]


def total(x, axis, n):
    for bit in bits_of(n):
        x = x + flip(x, bit, n, axis)
    return x


def dot_rows(left, right):
    return lax.dot_general(left, right, (((1,), (1,)), ((), ())), preferred_element_type=jnp.float32)


def held(x):
    return pl.BlockSpec(x.shape, lambda *_: (0,) * x.ndim, pipeline_mode=pl.Buffered(1))


def grams(pairs):
    given = []
    for pair in pairs:
        for block in pair:
            if not any(block is g for g in given):
                given.append(block)
    at = lambda block: next(i for i, g in enumerate(given) if g is block)
    flat = [x for block in given for x in block]
    rows = flat[0].shape[0]

    def kernel(*refs):
        out = refs[-1]
        for p, (left, right) in enumerate(pairs):
            i, j = 2 * at(left), 2 * at(right)

            @pl.when(pl.program_id(0) == p)
            def _():
                out[0] = dot_rows(refs[i][...], refs[j][...]) + dot_rows(refs[i + 1][...], refs[j + 1][...])

    width = sum(x.shape[1] for x in given[0])
    return pl.pallas_call(
        kernel,
        grid=(len(pairs),),
        in_specs=[held(x) for x in flat],
        out_specs=pl.BlockSpec((1, rows, rows), lambda p: (p, 0, 0)),
        out_shape=jax.ShapeDtypeStruct((len(pairs), rows, rows), jnp.float32),
        cost_estimate=pl.CostEstimate(
            flops=2 * len(pairs) * rows * rows * width,
            bytes_accessed=2 * len(flat) * flat[0].size + 4 * len(pairs) * rows * rows,
            transcendentals=0,
        ),
    )(*flat)


def products(gram, picks, blocks, base=None, tail=None):
    rows = gram.shape[1]
    tile = rows // 2 if rows % 32 == 0 else rows
    flat = [x for block in blocks for x in block]
    cut = blocks[0][0].shape[1]
    width = cut + blocks[0][1].shape[1]
    n = len(blocks)
    by_rows = pl.BlockSpec((tile, width), lambda m: (m, 0))
    specs = [pl.BlockSpec((gram.shape[0], tile, rows), lambda m: (0, m, 0))] + [held(x) for x in flat]
    args = [gram, *flat]
    if base is not None:
        specs.append(by_rows)
        args.append(base)
    if tail is not None:
        specs += [by_rows, pl.BlockSpec(memory_space=pltpu.SMEM)]
        args += tail

    def kernel(g, *refs):
        x, rest, out = refs[: 2 * n], list(refs[2 * n : -1]), refs[-1]
        for k, columns in enumerate((slice(0, cut), slice(cut, width))):
            value = None if base is None else rest[0][:, columns]
            for j, pick in enumerate(picks):
                term = jnp.dot(g[pick], x[2 * j + k][...], preferred_element_type=jnp.float32)
                value = term if value is None else value + term
            if tail is not None:
                normed = rest[-2][:, columns] / rest[-1][0, 0]
                value = (1.5 * normed - 0.5 * value) * jnp.sqrt(jnp.float32(3 * FF_WIN))
            out[:, columns] = value

    return pl.pallas_call(
        kernel,
        grid=(rows // tile,),
        in_specs=specs,
        out_specs=by_rows,
        out_shape=jax.ShapeDtypeStruct((rows, width), jnp.float32),
        cost_estimate=pl.CostEstimate(
            flops=2 * n * rows * rows * width,
            bytes_accessed=2 * n * rows * (rows + width) + 4 * rows * width,
            transcendentals=0,
        ),
    )(*args)


def scatter_sum(parts, me, n):
    for bit in bits_of(n):
        rows = parts.shape[1] // 2
        high = (me & bit) // bit
        take = lambda which: lax.dynamic_slice_in_dim(parts, which * rows, rows, 1)
        got = flip(take(1 - high), bit, n, "col")
        parts = take(high) + got
    return parts.astype(jnp.bfloat16)


def gather_rows(parts, me, n):
    for bit in reversed(bits_of(n)):
        other = flip(parts, bit, n, "col")
        low = (me & bit) == 0
        parts = jnp.concatenate([jnp.where(low, parts, other), jnp.where(low, other, parts)], 1)
    return parts


def solution(mesh):
    rows, cols = mesh.shape["row"], mesh.shape["col"]
    order = cycle(mesh)
    ahead = [(order[i], order[(i + 1) % rows]) for i in range(rows)]
    back = [(b, a) for a, b in ahead]
    far = rows // 2
    near = far // 2
    moved = lambda by: [(order[i], order[(i + by) % rows]) for i in range(rows)]

    def step_of(momentum, gradient):
        new_momentum = 0.95 * momentum + gradient
        squares = total(total(jnp.sum(new_momentum * new_momentum), "col", cols), "row", rows)
        norm = jnp.sqrt(3.0 * squares / D) + 1e-07
        normed = new_momentum / norm
        me = lax.axis_index("col")
        half = -(-normed.shape[1] // 256) * 128
        own = (normed[:, :half].astype(jnp.bfloat16), normed[:, half:].astype(jnp.bfloat16))
        blocks = {0: own}
        for d in range(1, far):
            for side, ring in ((-d, ahead), (d, back)):
                last = blocks[side + 1 if side < 0 else side - 1]
                got = []
                for k in (0, 1):
                    got.append(lax.ppermute(last[k], "row", ring))
                blocks[side] = tuple(got)
        last_a = lax.ppermute(blocks[1 - far][0], "row", ahead)
        last_b = lax.ppermute(blocks[far - 1][1], "row", back)
        blocks[far] = (last_a, last_b)

        crossing = [
            ((-(near - 1), near), -(near - 1), far - 1),
            ((near - 1, -near), near - 1, 1 - far),
            ((-near, near), -near, far),
        ]
        direct = {1: [0, -1, 1]} | {d: [-d, d] for d in range(2, far - 1)}
        shares = {}
        for d, js in direct.items():
            if d == near:
                shares["x"] = scatter_sum(grams([(blocks[i], blocks[j]) for (i, j), _, _ in crossing]), me, cols)
            shares[d] = scatter_sum(grams([(own, blocks[j]) for j in js]), me, cols)
        crossed = []
        for i, (_, by, j) in enumerate(crossing):
            crossed.append(lax.ppermute(shares["x"][i : i + 1], "row", moved(by)))
        total_so_far = None
        for d, js in direct.items():
            gram = gather_rows(shares[d], me, cols)
            total_so_far = products(gram, range(len(js)), [blocks[j] for j in js], total_so_far)
        gram = gather_rows(jnp.concatenate(crossed, 0), me, cols)
        total_so_far = products(gram, (0, 1), [blocks[far - 1], blocks[1 - far]], total_so_far)
        update = products(gram, (2,), [blocks[far]], total_so_far, (new_momentum, norm.reshape(1, 1)))
        return (new_momentum, update)

    placed = (P("row", "col"), P("row", "col"))
    return jax.shard_map(step_of, mesh=mesh, in_specs=placed, out_specs=placed, check_vma=False)
```

```python
import jax
import jax.numpy as jnp
from jax import lax
from jax.experimental import pallas as pl
from jax.experimental.pallas import tpu as pltpu
from jax.sharding import PartitionSpec as P


D = 5120
FF_WIN = 13312


def cycle(mesh):
    places = [tuple(d.coords) for d in mesh.devices[:, 0]]
    n = len(places)
    first = [a != b for a, b in zip(places[0], places[1 % n])]
    minor = n
    for i, place in enumerate(places):
        if any(a != b and not f for a, b, f in zip(place, places[0], first)):
            minor = i
            break
    major = n // minor
    order = []
    for i in range(major):
        along = range(1, minor) if i % 2 == 0 else range(minor - 1, 0, -1)
        order += [i * minor + j for j in along]
    order += [i * minor for i in range(major - 1, -1, -1)]
    return order


def flip(x, bit, n, axis):
    return lax.ppermute(x, axis, [(i, i ^ bit) for i in range(n)])


def bits_of(n):
    return [1 << k for k in range(n.bit_length() - 1)]


def total(x, axis, n):
    for bit in bits_of(n):
        x = x + flip(x, bit, n, axis)
    return x


def dot_rows(left, right):
    return lax.dot_general(left, right, (((1,), (1,)), ((), ())), preferred_element_type=jnp.float32)


def into(block, dst, sems):
    at, copies = 0, []
    for i, piece in enumerate(block):
        wide = piece.shape[1]
        copies.append(pltpu.make_async_copy(piece, dst.at[:, at : at + wide], sems.at[i]))
        at += wide
    return copies


ANY = pl.BlockSpec(memory_space=pl.ANY)


def grams(pairs, high):
    given = []
    for pair in pairs:
        for block in pair:
            if not any(block is g for g in given):
                given.append(block)
    at = lambda block: next(i for i, g in enumerate(given) if g is block)
    flat = [x for block in given for x in block]
    rows, half = flat[0].shape[0], flat[0].shape[0] // 2
    width = sum(x.shape[1] for x in given[0])
    same = all(left is pairs[0][0] for left, _ in pairs)

    def kernel(high_ref, *refs):
        kept, sent, left, right, sems = refs[len(flat) :]
        block = lambda b: refs[2 * at(b) : 2 * at(b) + 2]

        def copies(p):
            got = into(block(pairs[p][1]), right.at[p % 2], sems.at[p % 2, 0])
            if p == 0 or not same:
                got += into(block(pairs[p][0]), left.at[p % 2], sems.at[p % 2, 1])
            return got

        step = pl.program_id(0)
        for p in range(len(pairs)):

            @pl.when(step == p)
            def _():
                for q in (0, 1) if p == 0 else (p + 1,):
                    if q < len(pairs):
                        for c in copies(q):
                            c.start()
                for c in copies(p):
                    c.wait()

        slot = lax.rem(step, 2)
        value = dot_rows(left[0 if same else slot], right[slot])

        @pl.when(high_ref[0] == 0)
        def _():
            kept[0] = value[:half]
            sent[0] = value[half:]

        @pl.when(high_ref[0] != 0)
        def _():
            kept[0] = value[half:]
            sent[0] = value[:half]

    out = pl.BlockSpec((1, half, rows), lambda p: (p, 0, 0))
    return pl.pallas_call(
        kernel,
        grid=(len(pairs),),
        in_specs=[pl.BlockSpec(memory_space=pltpu.SMEM)] + [ANY] * len(flat),
        out_specs=(out, out),
        out_shape=(jax.ShapeDtypeStruct((len(pairs), half, rows), jnp.float32),) * 2,
        scratch_shapes=[
            pltpu.VMEM((1 if same else 2, rows, width), jnp.bfloat16),
            pltpu.VMEM((2, rows, width), jnp.bfloat16),
            pltpu.SemaphoreType.DMA((2, 2, 2)),
        ],
        cost_estimate=pl.CostEstimate(
            flops=2 * len(pairs) * rows * rows * width,
            bytes_accessed=2 * len(flat) * flat[0].size + 4 * len(pairs) * rows * rows,
            transcendentals=0,
        ),
    )(high.reshape(1), *flat)


def products(gram, picks, blocks, high, base=None, tail=None, scale=1.0, cuts=1):
    n = len(blocks)
    half, rows = gram[0].shape[1:]
    flat = [x for block in blocks for x in block]
    width = sum(x.shape[1] for x in blocks[0])
    cuts = cuts if half % (16 * cuts) == 0 else 1
    tile = half // cuts
    by_rows = pl.BlockSpec((tile, width), lambda m, hi: (cuts * ((m // cuts + hi[0]) % 2) + m % cuts, 0))
    specs = [ANY] * (2 + len(flat))
    args = [*gram, *flat]
    if base is not None:
        specs.append(by_rows)
        args.append(base)
    if tail is not None:
        specs += [by_rows, pl.BlockSpec(memory_space=pltpu.SMEM)]
        args += tail

    def kernel(_, mine, other, *refs):
        pieces, rest = refs[: 2 * n], refs[2 * n : -5]
        out, g, x, g_sems, x_sems = refs[-5:]
        m = pl.program_id(0)

        def copies(j):
            halves = [
                pltpu.make_async_copy(src.at[picks[j]], g.at[i, j], g_sems.at[i, j]) for i, src in enumerate((mine, other))
            ]
            return halves + into(pieces[2 * j : 2 * j + 2], x.at[j], x_sems.at[j])

        @pl.when(m == 0)
        def _():
            for j in range(n):
                for c in copies(j):
                    c.start()

        out[...] = jnp.zeros_like(out) if base is None else rest[0][...]

        def add(j, carry):
            for i in range(n):

                @pl.when((m == 0) & (j == i))
                def _():
                    for c in copies(i):
                        c.wait()

            here = pl.ds(pl.multiple_of(lax.rem(m, cuts) * tile, tile), tile)
            out[...] += scale * jnp.dot(g[m // cuts, j, here, :], x[j], preferred_element_type=jnp.float32)
            return carry

        lax.fori_loop(0, n, add, 0)
        if tail is not None:
            normed = rest[-2][...] / rest[-1][0, 0]
            out[...] = (1.5 * normed - 0.5 * out[...]) * jnp.sqrt(jnp.float32(3 * FF_WIN))

    return pl.pallas_call(
        kernel,
        grid_spec=pltpu.PrefetchScalarGridSpec(
            num_scalar_prefetch=1,
            grid=(2 * cuts,),
            in_specs=specs,
            out_specs=by_rows,
            scratch_shapes=[
                pltpu.VMEM((2, n, half, rows), jnp.bfloat16),
                pltpu.VMEM((n, rows, width), jnp.bfloat16),
                pltpu.SemaphoreType.DMA((2, n)),
                pltpu.SemaphoreType.DMA((n, 2)),
            ],
        ),
        out_shape=jax.ShapeDtypeStruct((rows, width), jnp.float32),
        cost_estimate=pl.CostEstimate(
            flops=2 * n * rows * rows * width,
            bytes_accessed=2 * n * rows * (rows + width) + 4 * rows * width,
            transcendentals=0,
        ),
    )(high.reshape(1), *args)


def scatter_sum(halves, me, n):
    kept, sent = halves
    for bit in bits_of(n):
        if bit > 1:
            rows = parts.shape[1] // 2
            high = (me & bit) // bit
            sent = lax.dynamic_slice_in_dim(parts, (1 - high) * rows, rows, 1)
            kept = lax.dynamic_slice_in_dim(parts, high * rows, rows, 1)
        parts = kept + flip(sent, bit, n, "col")
    return parts.astype(jnp.bfloat16)


def gather_rows(parts, me, n):
    for bit in reversed(bits_of(n)):
        other = flip(parts, bit, n, "col")
        if bit > 1:
            low = (me & bit) == 0
            parts = jnp.concatenate([jnp.where(low, parts, other), jnp.where(low, other, parts)], 1)
    return parts, other


def solution(mesh):
    rows, cols = mesh.shape["row"], mesh.shape["col"]
    order = cycle(mesh)
    ahead = [(order[i], order[(i + 1) % rows]) for i in range(rows)]
    back = [(b, a) for a, b in ahead]
    far = rows // 2
    near = far // 2
    moved = lambda by: [(order[i], order[(i + by) % rows]) for i in range(rows)]

    def step_of(momentum, gradient):
        new_momentum = 0.95 * momentum + gradient
        squares = total(total(jnp.sum(new_momentum * new_momentum), "col", cols), "row", rows)
        norm = jnp.sqrt(3.0 * squares / D) + 1e-07
        normed = new_momentum / norm
        me = lax.axis_index("col")
        high = (me & 1).astype(jnp.int32)
        half = -(-normed.shape[1] // 256) * 128
        own = (normed[:, :half].astype(jnp.bfloat16), normed[:, half:].astype(jnp.bfloat16))
        blocks = {0: own}
        for d in range(1, far):
            for side, ring in ((-d, ahead), (d, back)):
                last = blocks[side + 1 if side < 0 else side - 1]
                got = []
                for k in (0, 1):
                    got.append(lax.ppermute(last[k], "row", ring))
                blocks[side] = tuple(got)
        last_a = lax.ppermute(blocks[1 - far][0], "row", ahead)
        last_b = lax.ppermute(blocks[far - 1][1], "row", back)
        blocks[far] = (last_a, last_b)

        crossing = [
            ((-(near - 1), near), -(near - 1), far - 1),
            ((near - 1, -near), near - 1, 1 - far),
            ((-near, near), -near, far),
        ]
        direct = {1: [0, -1, 1]} | {d: [-d, d] for d in range(2, far - 1)}
        shares = {}
        for d, js in direct.items():
            shares[d] = scatter_sum(grams([(own, blocks[j]) for j in js], high), me, cols)
            if d == near:
                pairs = [(blocks[i], blocks[j]) for (i, j), _, _ in crossing]
                shares["x"] = scatter_sum(grams(pairs, high), me, cols)
        crossed = []
        for i, (_, by, j) in enumerate(crossing):
            crossed.append(lax.ppermute(shares["x"][i : i + 1], "row", moved(by)))
        totals = [None]
        for d, js in direct.items():
            gram = gather_rows(shares[d], me, cols)
            totals.append(products(gram, range(len(js)), [blocks[j] for j in js], high, totals[-1]))
        crossed, _ = lax.optimization_barrier((jnp.concatenate(crossed, 0), totals[1]))
        gram = gather_rows(crossed, me, cols)
        most = products(
            gram, (0, 1), [blocks[far - 1], blocks[1 - far]], high, totals[-1], (new_momentum, norm.reshape(1, 1))
        )
        scale = -0.5 * (3 * FF_WIN) ** 0.5
        update = products(gram, (2,), [blocks[far]], high, most, scale=scale, cuts=2)
        return (new_momentum, update)

    placed = (P("row", "col"), P("row", "col"))
    return jax.shard_map(step_of, mesh=mesh, in_specs=placed, out_specs=placed, check_vma=False)
```
